32 devices in a mesh: dp: 4 (over x, y), ep: 8 (over z, core).
Axes of the slice: x: 2, y: 2, z: 4, core: 2. Of those that a mesh axis runs over, the one named last changes fastest.
Arguments:
- x: bfloat16 [4, 8, 256, 3584], P('dp', 'ep'), parts along dimension 0
- expert: int32 [4, 8, 256, 8], P('dp', 'ep'), parts along dimension 0
- slot: int32 [4, 8, 256, 8], P('dp', 'ep'), parts along dimension 0
- gate: float32 [4, 8, 256, 8], P('dp', 'ep'), parts along dimension 0
- w_gate: bfloat16 [32, 3584, 2560], P('ep')
- w_up: bfloat16 [32, 3584, 2560], P('ep')
- w_down: bfloat16 [32, 2560, 3584], P('ep')
- s_gate: bfloat16 [3584, 20480], replicated
- s_up: bfloat16 [3584, 20480], replicated
- s_down: bfloat16 [20480, 3584], replicated
Outputs:
- y: bfloat16 [4, 8, 256, 3584], P('dp', 'ep'), parts along dimension 0
There are 4 independent parts. The reference program is written for one: setup_inputs(seed, part) draws one part's arguments, and reference() takes and returns one part's arrays. A program takes and returns all parts, laid end to end along the dimension named above; an argument that names none is the same for every part.
All inputs are finite; a program needn't handle non-finite values.
Results may differ from the reference program's by a relative error of at most 0.009.
Values are sent between devices in bfloat16 or wider.
A program may use at most 2 GiB of HBM per device.

```python
import jax
import jax.numpy as jnp

MEMBERS = 8
TOKENS = 256
D = 3584
FF = 2560
TOP = 8
EXPERTS = 32
SHARED_FF = 20480
SLOTS = 5 * TOKENS * TOP // (4 * EXPERTS)


def setup_inputs(seed: int = 0, part: int = 0) -> dict:
    own, k1, k2, k3, k4, k5, k6 = jax.random.split(jax.random.key(seed), 7)
    kx, ke, kl, kg = jax.random.split(jax.random.fold_in(own, part), 4)
    devices = (1, MEMBERS)
    place = jax.random.permutation(kl, jnp.arange(EXPERTS, dtype=jnp.uint32))
    slow = ((EXPERTS + (9 * place) % EXPERTS) << ((9 * place) // EXPERTS)) // EXPERTS
    wait = (jax.random.bits(ke, (*devices, TOKENS, EXPERTS), jnp.uint32) >> 10) * slow
    expert = jnp.argsort(wait, axis=-1)[..., :TOP].astype(jnp.int32)
    chosen = jax.nn.one_hot(expert, EXPERTS, dtype=jnp.int32)
    in_line = jnp.cumsum(chosen.reshape(*devices, TOKENS * TOP, EXPERTS), axis=2) - 1
    slot = jnp.sum(in_line.reshape(chosen.shape) * chosen, axis=-1)

    def one(key, rows, columns):
        return (jax.random.normal(key, (rows, columns), jnp.float32) * rows**-0.5).astype(jnp.bfloat16)

    def weights(key, rows, columns):
        return jax.lax.map(lambda k: one(k, rows, columns), jax.random.split(key, EXPERTS))

    return {
        "x": jax.random.normal(kx, (*devices, TOKENS, D), jnp.float32).astype(jnp.bfloat16),
        "expert": expert,
        "slot": slot,
        "gate": jax.nn.softmax(jax.random.normal(kg, expert.shape, jnp.float32)),
        "w_gate": weights(k1, D, FF),
        "w_up": weights(k2, D, FF),
        "w_down": weights(k3, FF, D),
        "s_gate": one(k4, D, SHARED_FF),
        "s_up": one(k5, D, SHARED_FF),
        "s_down": one(k6, SHARED_FF, D),
    }


def einsum(form, a, b):
    return jnp.einsum(form, a.astype(jnp.float32), b.astype(jnp.float32))


def for_all(x, s_gate, s_up, s_down):
    h = jax.nn.silu(einsum("...d,df->...f", x, s_gate)) * einsum("...d,df->...f", x, s_up)
    return einsum("...f,fd->...d", h.astype(jnp.bfloat16), s_down)


def reference(x, expert, slot, gate, w_gate, w_up, w_down, s_gate, s_up, s_down):
    to_expert = jax.nn.one_hot(expert, EXPERTS, dtype=jnp.bfloat16)
    to_slot = jax.nn.one_hot(slot, SLOTS, dtype=jnp.bfloat16)
    weighted = to_expert * gate[..., None].astype(jnp.bfloat16)
    dispatch = einsum("abtke,abtkc->abtec", to_expert, to_slot).astype(jnp.bfloat16)
    combine = einsum("abtke,abtkc->abtec", weighted, to_slot).astype(jnp.bfloat16)
    z = einsum("abtec,abtd->aebcd", dispatch, x).astype(jnp.bfloat16)
    h = jax.nn.silu(einsum("aebcd,edf->aebcf", z, w_gate))
    h = (h * einsum("aebcd,edf->aebcf", z, w_up)).astype(jnp.bfloat16)
    out = einsum("aebcf,efd->aebcd", h, w_down).astype(jnp.bfloat16)
    y = einsum("abtec,aebcd->abtd", combine, out)
    return (y + for_all(x, s_gate, s_up, s_down)).astype(jnp.bfloat16)
```

```python
import functools

import jax
import jax.numpy as jnp
from jax import lax
from jax.experimental import pallas as pl
from jax.experimental.pallas import tpu as pltpu
from jax.sharding import PartitionSpec as P

BF = jnp.bfloat16
F32 = jnp.float32
FN = 512
CHUNKS = 2
GROUP = 16
PARAMS = dict(vmem_limit_bytes=67_043_328)


def dot(a, b):
    return jnp.dot(a, b, preferred_element_type=F32)


def gated(z, wg, wu):
    g = dot(z, wg)
    return (g * jax.nn.sigmoid(g) * dot(z, wu)).astype(BF)


def weight_specs(experts, ff, d, first=0, stacked=True):
    ups = ff // FN

    def up(e, s, *_):
        last = e == experts - 1
        block = jnp.where(s < ups, s, jnp.where(last, ups - 1, 0))
        which = jnp.where((s < ups) | last, e, e + 1) + first
        return (which, 0, block) if stacked else (0, which * ups + block)

    def down(e, s, *_):
        n = jnp.maximum(s - ups, 0)
        return (e + first, 0, n) if stacked else (e + first, n)

    lead = (1,) if stacked else ()
    return [
        pl.BlockSpec((*lead, d, FN), up),
        pl.BlockSpec((*lead, d, FN), up),
        pl.BlockSpec((*lead, ff, FN), down),
    ]


def shared_kernel(ups, x_ref, wg_ref, wu_ref, wd_ref, y_ref, h_ref):
    g, s = pl.program_id(0), pl.program_id(1)

    @pl.when(s < ups)
    def _():
        at = pl.ds(pl.multiple_of(s * FN, FN), FN)
        h_ref[:, at] = gated(x_ref[...], wg_ref[...], wu_ref[...])

    @pl.when(s >= ups)
    def _():
        at = pl.ds(pl.multiple_of((s - ups) * FN, FN), FN)
        out = dot(h_ref[...], wd_ref[...])

        @pl.when(g == 0)
        def _():
            y_ref[:, at] = out

        @pl.when(g > 0)
        def _():
            y_ref[:, at] += out


def shared(x, s_gate, s_up, s_down, ff, first, groups):
    tokens, d = x.shape
    ups, downs = ff // FN, d // FN
    return pl.pallas_call(
        functools.partial(shared_kernel, ups),
        grid=(groups, ups + downs),
        in_specs=[pl.BlockSpec((tokens, d), lambda g, s: (0, 0))]
        + weight_specs(groups, ff, d, first, stacked=False),
        out_specs=pl.BlockSpec((tokens, d), lambda g, s: (0, 0)),
        out_shape=jax.ShapeDtypeStruct((tokens, d), F32),
        scratch_shapes=[pltpu.VMEM((tokens, ff), BF)],
        compiler_params=pltpu.CompilerParams(**PARAMS),
        cost_estimate=pl.CostEstimate(
            flops=6 * tokens * d * ff * groups,
            bytes_accessed=6 * d * ff * groups,
            transcendentals=0,
        ),
        name="shared",
    )(x, s_gate, s_up, s_down)


def routed_kernel(ups, sizes, count_ref, x_ref, row_ref, col_ref, wg_ref, wu_ref, wd_ref,
                  out_ref, y_ref, z_ref, h_ref, c_ref):
    e, s = pl.program_id(0), pl.program_id(1)
    tokens = x_ref.shape[0]
    count = count_ref[e]

    @pl.when((e == 0) & (s == 0))
    def _():
        y_ref[...] = jnp.zeros_like(y_ref)

    below = 0
    for m in sizes:
        here = (count > below) & (count <= m)
        below = m

        @pl.when(here & (s == 0))
        def _():
            hit = row_ref[0] == lax.broadcasted_iota(jnp.int32, (m, tokens), 0).astype(F32)
            pick = jnp.where(hit, 1.0, 0.0).astype(BF)

            @pl.loop(0, x_ref.shape[1] // FN)
            def _(n):
                at = pl.ds(pl.multiple_of(n * FN, FN), FN)
                z_ref[:m, at] = dot(pick, x_ref[:, at]).astype(BF)

            spot = lax.broadcasted_iota(jnp.int32, (tokens, m), 1).astype(F32)
            c_ref[:, :m] = jnp.where(col_ref[0, :, 0:1] == spot, col_ref[0, :, 1:2], 0.0).astype(BF)

        @pl.when(here & (s < ups))
        def _():
            at = pl.ds(pl.multiple_of(s * FN, FN), FN)
            h_ref[:m, at] = gated(z_ref[:m, :], wg_ref[0], wu_ref[0])

        @pl.when(here & (s >= ups))
        def _():
            at = pl.ds(pl.multiple_of((s - ups) * FN, FN), FN)
            out = dot(h_ref[:m, :], wd_ref[0]).astype(BF)
            y_ref[:, at] += dot(c_ref[:, :m], out)

    @pl.when((e == pl.num_programs(0) - 1) & (s >= ups))
    def _():
        at = pl.ds(pl.multiple_of((s - ups) * FN, FN), FN)
        out_ref[...] = y_ref[:, at].astype(BF)


def routed(count, x, row, col, w_gate, w_up, w_down, most):
    (tokens, d), (experts, _, ff) = x.shape, w_gate.shape
    ups, downs = ff // FN, d // FN
    sizes = tuple(range(128, most, 128)) + (most,)

    def tile(e, s, *_):
        return (0, jnp.where(e == experts - 1, jnp.maximum(s - ups, 0), 0))

    return pl.pallas_call(
        functools.partial(routed_kernel, ups, sizes),
        grid_spec=pltpu.PrefetchScalarGridSpec(
            num_scalar_prefetch=1,
            grid=(experts, ups + downs),
            in_specs=[
                pl.BlockSpec((tokens, d), lambda e, s, *_: (0, 0), pipeline_mode=pl.Buffered(1)),
                pl.BlockSpec((1, 1, tokens), lambda e, s, *_: (e, 0, 0)),
                pl.BlockSpec((1, tokens, 2), lambda e, s, *_: (e, 0, 0)),
            ]
            + weight_specs(experts, ff, d),
            out_specs=pl.BlockSpec((tokens, FN), tile),
            scratch_shapes=[
                pltpu.VMEM((tokens, d), F32),
                pltpu.VMEM((most, d), BF),
                pltpu.VMEM((most, ff), BF),
                pltpu.VMEM((tokens, most), BF),
            ],
        ),
        out_shape=jax.ShapeDtypeStruct((tokens, d), BF),
        compiler_params=pltpu.CompilerParams(**PARAMS),
        cost_estimate=pl.CostEstimate(
            flops=6 * most * d * ff * experts // 2,
            bytes_accessed=6 * d * ff * experts,
            transcendentals=0,
        ),
        name="routed",
    )(count, x, row, col, w_gate, w_up, w_down)


def solution(mesh):
    members = mesh.shape["ep"]

    def local(x, expert, slot, gate, w_gate, w_up, w_down, s_gate, s_up, s_down):
        x, expert, slot, gate = (v[0, 0] for v in (x, expert, slot, gate))
        (tokens, d), top = x.shape, expert.shape[1]
        mine, _, ff = w_gate.shape
        experts = mine * members
        slots = 5 * tokens * top // (4 * experts)
        part = tokens // CHUNKS
        most = min(members * slots, members * part)
        me = lax.axis_index("ep")

        deal = x.reshape(part // GROUP, CHUNKS, GROUP, d)
        xs = [deal[:, c].reshape(part, d) for c in range(CHUNKS)]
        xs = [lax.all_gather(v, "ep").reshape(members * part, d) for v in xs]

        hit = (expert[None] == jnp.arange(experts)[:, None, None]) & (slot < slots)[None]
        weight = gate.astype(BF).astype(F32)
        meta = jnp.concatenate(
            [jnp.any(hit, -1).astype(F32), jnp.sum(jnp.where(hit, weight[None], 0.0), -1)]
        ).astype(BF)
        meta = lax.all_gather(meta.reshape(2, experts, tokens), "ep")
        meta = lax.dynamic_slice_in_dim(meta, me * mine, mine, 2).astype(F32)
        meta = meta.reshape(members, 2, mine, part // GROUP, CHUNKS, GROUP)
        meta = meta.transpose(4, 1, 2, 0, 3, 5).reshape(CHUNKS, 2, mine, members * part)
        chosen, weight = meta[:, 0], meta[:, 1]
        rank = jnp.cumsum(chosen, -1)
        count = rank[..., -1].astype(jnp.int32)
        rank = jnp.where(chosen > 0, rank - 1, -1.0)
        row = rank[:, :, None, :]
        col = jnp.stack([rank, weight], -1)

        half = s_gate.shape[1] // ff // 2
        rest = s_gate.shape[1] // ff - half
        sh = shared(x, s_gate, s_up, s_down, ff, 0, half)
        (sh, xs[0]) = lax.optimization_barrier((sh, xs[0]))
        sums = []
        for c in range(CHUNKS):
            y = routed(count[c], xs[c], row[c], col[c], w_gate, w_up, w_down, most)
            if c + 1 < CHUNKS:
                y, xs[c + 1] = lax.optimization_barrier((y, xs[c + 1]))
            else:
                y, x = lax.optimization_barrier((y, x))
            sums.append(lax.psum_scatter(y.reshape(members, part, d), "ep"))
        sh2 = shared(x, s_gate, s_up, s_down, ff, half, rest)
        y = jnp.stack([v.reshape(part // GROUP, GROUP, d) for v in sums], 1).reshape(tokens, d)
        y = y.astype(F32) + (sh + sh2)
        return y.astype(BF)[None, None]

    held = P("dp", "ep", None, None)
    split, whole = P("ep", None, None), P(None, None)
    return jax.shard_map(
        local,
        mesh=mesh,
        in_specs=(held,) * 4 + (split,) * 3 + (whole,) * 3,
        out_specs=held,
        check_vma=False,
    )
```

```python
import functools

import jax
import jax.numpy as jnp
from jax import lax
from jax.experimental import pallas as pl
from jax.experimental.pallas import tpu as pltpu
from jax.sharding import PartitionSpec as P

BF = jnp.bfloat16
F32 = jnp.float32
UP, DOWN = 256, 512
CHUNKS = 2
GROUP = 16
LANES = 128
SIZES = (128, 192, 256, 320, 384)
PARAMS = dict(vmem_limit_bytes=67_043_328)
ANY = pl.BlockSpec(memory_space=pl.ANY)


def dot(a, b):
    return jnp.dot(a, b, preferred_element_type=F32)


def gated(z, wg, wu):
    g = dot(z, wg)
    return (g * jax.nn.sigmoid(g) * dot(z, wu)).astype(BF)


def span(i, size):
    return pl.ds(pl.multiple_of(i * size, size), size)


class Stream:
    def __init__(self, sources, buf, sem, count):
        self.sources, self.buf, self.sem, self.count = sources, buf, sem, count
        self.slots = buf.shape[0]

    def copies(self, i):
        slot = lax.rem(i, self.slots)
        return [
            pltpu.make_async_copy(ref, self.buf.at[slot, k], self.sem.at[slot, k])
            for k, ref in enumerate(self.sources(i))
        ]

    def begin(self):
        for i in range(min(self.slots, self.count)):
            for copy in self.copies(jnp.int32(i)):
                copy.start()

    def take(self, i):
        for copy in self.copies(i):
            copy.wait()
        return self.buf.at[lax.rem(i, self.slots)]

    def free(self, i):
        @pl.when(i + self.slots < self.count)
        def _():
            for copy in self.copies(i + self.slots):
                copy.start()


def shared_kernel(first, groups, ff, x_ref, wg_ref, wu_ref, wd_ref, y_ref, h_ref, ubuf, usem, dbuf, dsem):
    d = x_ref.shape[1]
    ups, downs = ff // UP, d // DOWN

    def up(i):
        at = span(first * ups + i, UP)
        return wg_ref.at[:, at], wu_ref.at[:, at]

    def down(i):
        return (wd_ref.at[span(first + i // downs, ff), span(lax.rem(i, downs), DOWN)],)

    us = Stream(up, ubuf, usem, groups * ups)
    ds = Stream(down, dbuf, dsem, groups * downs)
    us.begin()
    ds.begin()
    y_ref[...] = jnp.zeros_like(y_ref)

    @pl.loop(0, groups)
    def _(g):
        @pl.loop(0, ups)
        def _(s):
            i = g * ups + s
            w = us.take(i)
            h_ref[:, span(s, UP)] = gated(x_ref[...], w[0], w[1])
            us.free(i)

        @pl.loop(0, downs)
        def _(n):
            i = g * downs + n
            w = ds.take(i)
            y_ref[:, span(n, DOWN)] += dot(h_ref[...], w[0])
            ds.free(i)


def shared(x, s_gate, s_up, s_down, ff, first, groups):
    tokens, d = x.shape
    return pl.pallas_call(
        functools.partial(shared_kernel, first, groups, ff),
        in_specs=[pl.BlockSpec(memory_space=pltpu.VMEM)] + [ANY] * 3,
        out_specs=pl.BlockSpec(memory_space=pltpu.VMEM),
        out_shape=jax.ShapeDtypeStruct((tokens, d), F32),
        scratch_shapes=[
            pltpu.VMEM((tokens, ff), BF),
            pltpu.VMEM((4, 2, d, UP), BF),
            pltpu.SemaphoreType.DMA((4, 2)),
            pltpu.VMEM((4, 1, ff, DOWN), BF),
            pltpu.SemaphoreType.DMA((4, 1)),
        ],
        compiler_params=pltpu.CompilerParams(**PARAMS),
        cost_estimate=pl.CostEstimate(
            flops=6 * tokens * d * ff * groups,
            bytes_accessed=6 * d * ff * groups,
            transcendentals=0,
        ),
        name="shared",
    )(x, s_gate, s_up, s_down)


def routed_kernel(experts, x_ref, wg_ref, wu_ref, wd_ref, out_ref, xv, note, rank_ref, col_ref,
                  y_ref, z_ref, h_ref, c_ref, sent, ubuf, usem, dbuf, dsem, xsem, osem):
    mine, d, ff = wg_ref.shape
    tokens = x_ref.shape[0]
    ups, downs = ff // UP, d // DOWN

    def up(i):
        e, at = i // ups, span(lax.rem(i, ups), UP)
        return wg_ref.at[e, :, at], wu_ref.at[e, :, at]

    def down(i):
        return (wd_ref.at[i // downs, :, span(lax.rem(i, downs), DOWN)],)

    def result(n):
        slot = lax.rem(n, 2)
        return pltpu.make_async_copy(sent.at[slot], out_ref.at[:, span(n, DOWN)], osem.at[slot])

    us = Stream(up, ubuf, usem, mine * ups)
    ds = Stream(down, dbuf, dsem, mine * downs)
    note_copy = pltpu.make_async_copy(x_ref.at[:, pl.ds(d, LANES)], note, xsem.at[0])
    x_copy = pltpu.make_async_copy(x_ref.at[:, pl.ds(0, d)], xv, xsem.at[1])
    note_copy.start()
    x_copy.start()
    us.begin()
    ds.begin()
    y_ref[...] = jnp.zeros_like(y_ref)

    me = lax.axis_index("ep") * mine
    k = lax.broadcasted_iota(jnp.int32, (LANES, LANES), 0)
    j = lax.broadcasted_iota(jnp.int32, (LANES, LANES), 1)
    wanted = jnp.where(j < mine, me + j, experts + me + j - mine)
    own = jnp.where((j < 2 * mine) & (k == wanted), 1.0, 0.0).astype(BF)
    note_copy.wait()
    cols = dot(note[...], own)
    before = lax.broadcasted_iota(jnp.int32, (tokens, tokens), 1) <= lax.broadcasted_iota(
        jnp.int32, (tokens, tokens), 0
    )
    upto = dot(jnp.where(before, 1.0, 0.0).astype(BF), cols.astype(BF))
    rank = jnp.where(cols > 0.5, upto - 1.0, -1.0)
    rank_ref[...] = rank.T
    for e in range(mine):
        col_ref[e, :, 0:1] = rank[:, e : e + 1]
        col_ref[e, :, 1:2] = cols[:, mine + e : mine + e + 1]
    x_copy.wait()

    @pl.loop(0, mine)
    def _(e):
        row = rank_ref[pl.ds(e, 1), :]
        count = jnp.max(row).astype(jnp.int32) + 1
        top = SIZES[-1]
        blocks = jnp.where(count > top, 2, 1)
        need = jnp.where(count > top, (count + 1) // 2, count)

        def each(body):
            below = 0
            for m in SIZES:

                @pl.when((need > below) & (need <= m))
                def _():
                    pl.loop(0, blocks)(functools.partial(body, m))

                below = m

        def dispatch(m, b):
            spot = lax.broadcasted_iota(jnp.int32, (m, tokens), 0) + b * m
            pick = jnp.where(row == spot.astype(F32), 1.0, 0.0).astype(BF)

            @pl.loop(0, downs)
            def _(n):
                at = span(n, DOWN)
                z_ref[span(b, m), at] = dot(pick, xv[:, at]).astype(BF)

            spot = lax.broadcasted_iota(jnp.int32, (tokens, m), 1) + b * m
            hit = col_ref[e, :, 0:1] == spot.astype(F32)
            c_ref[b, :, :m] = jnp.where(hit, col_ref[e, :, 1:2], 0.0).astype(BF)

        each(dispatch)

        @pl.loop(0, ups)
        def _(s):
            i = e * ups + s
            w = us.take(i)

            def body(m, b):
                h_ref[span(b, m), span(s, UP)] = gated(z_ref[span(b, m), :], w[0], w[1])

            each(body)
            us.free(i)

        @pl.loop(0, downs)
        def _(n):
            i = e * downs + n
            w = ds.take(i)
            at = span(n, DOWN)

            def body(m, b):
                out = dot(h_ref[span(b, m), :], w[0]).astype(BF)
                y_ref[:, at] += dot(c_ref[b, :, :m], out)

            each(body)
            ds.free(i)

            @pl.when(e == mine - 1)
            def _():
                @pl.when(n >= 2)
                def _():
                    result(n - 2).wait()

                sent[lax.rem(n, 2)] = y_ref[:, at].astype(BF)
                result(n).start()

    for n in range(max(downs - 2, 0), downs):
        result(jnp.int32(n)).wait()


def routed(x, w_gate, w_up, w_down, experts, most):
    tokens, (mine, d, ff) = x.shape[0], w_gate.shape
    top = SIZES[-1]
    rows = 2 * SIZES[-2]
    assert most <= rows
    return pl.pallas_call(
        functools.partial(routed_kernel, experts),
        in_specs=[ANY] * 4,
        out_specs=ANY,
        scratch_shapes=[
            pltpu.VMEM((tokens, d), BF),
            pltpu.VMEM((tokens, LANES), BF),
            pltpu.VMEM((LANES, tokens), F32),
            pltpu.VMEM((mine, tokens, 2), F32),
            pltpu.VMEM((tokens, d), F32),
            pltpu.VMEM((rows, d), BF),
            pltpu.VMEM((rows, ff), BF),
            pltpu.VMEM((2, tokens, top), BF),
            pltpu.VMEM((2, tokens, DOWN), BF),
            pltpu.VMEM((3, 2, d, UP), BF),
            pltpu.SemaphoreType.DMA((3, 2)),
            pltpu.VMEM((2, 1, ff, DOWN), BF),
            pltpu.SemaphoreType.DMA((2, 1)),
            pltpu.SemaphoreType.DMA((2,)),
            pltpu.SemaphoreType.DMA((2,)),
        ],
        out_shape=jax.ShapeDtypeStruct((tokens, d), BF),
        compiler_params=pltpu.CompilerParams(**PARAMS),
        cost_estimate=pl.CostEstimate(
            flops=6 * most * d * ff * mine // 2,
            bytes_accessed=6 * d * ff * mine,
            transcendentals=0,
        ),
        name="routed",
    )(x, w_gate, w_up, w_down)


def solution(mesh):
    members = mesh.shape["ep"]

    def local(x, expert, slot, gate, w_gate, w_up, w_down, s_gate, s_up, s_down):
        x, expert, slot, gate = (v[0, 0] for v in (x, expert, slot, gate))
        (tokens, d), top = x.shape, expert.shape[1]
        mine, _, ff = w_gate.shape
        experts = mine * members
        slots = 5 * tokens * top // (4 * experts)
        part = tokens // CHUNKS
        most = min(members * slots, members * part)

        hit = (expert[:, None, :] == jnp.arange(experts)[None, :, None]) & (slot < slots)[:, None, :]
        weight = gate.astype(BF).astype(F32)[:, None, :]
        note = jnp.concatenate(
            [
                jnp.any(hit, -1).astype(F32),
                jnp.sum(jnp.where(hit, weight, 0.0), -1),
                jnp.zeros((tokens, LANES - 2 * experts), F32),
            ],
            1,
        ).astype(BF)
        deal = jnp.concatenate([x, note], 1).reshape(part // GROUP, CHUNKS, GROUP, d + LANES)
        xs = [deal[:, c].reshape(part, d + LANES) for c in range(CHUNKS)]
        xs = [lax.all_gather(v, "ep").reshape(members * part, d + LANES) for v in xs]

        half = s_gate.shape[1] // ff // 2
        rest = s_gate.shape[1] // ff - half
        sh = shared(x, s_gate, s_up, s_down, ff, 0, half)
        (sh, xs[0]) = lax.optimization_barrier((sh, xs[0]))
        sums = []
        for c in range(CHUNKS):
            y = routed(xs[c], w_gate, w_up, w_down, experts, most)
            if c + 1 < CHUNKS:
                y, xs[c + 1] = lax.optimization_barrier((y, xs[c + 1]))
            else:
                y, x = lax.optimization_barrier((y, x))
            sums.append(lax.psum_scatter(y.reshape(members, part, d), "ep"))
        sh2 = shared(x, s_gate, s_up, s_down, ff, half, rest)
        y = jnp.stack([v.reshape(part // GROUP, GROUP, d) for v in sums], 1).reshape(tokens, d)
        y = y.astype(F32) + (sh + sh2)
        return y.astype(BF)[None, None]

    held = P("dp", "ep", None, None)
    split, whole = P("ep", None, None), P(None, None)
    return jax.shard_map(
        local,
        mesh=mesh,
        in_specs=(held,) * 4 + (split,) * 3 + (whole,) * 3,
        out_specs=held,
        check_vma=False,
    )
```
